32 devices in a mesh: rep: 16 (over z, y, core), grp: 2 (over x).
Axes of the slice: x: 2, y: 2, z: 4, core: 2. Of those that a mesh axis runs over, the one named last changes fastest.
Arguments:
- local_params: bfloat16 [16, 2, 32, 8192], P('rep', 'grp'), may hold values from -130 to 130
- snapshot: bfloat16 [2, 32, 8192], P('grp'), may hold values from -4 to 4
- master: float32 [2, 32, 8192], P('grp', 'rep'), may hold values from -6 to 6
- momentum: float32 [2, 32, 8192], P('grp', 'rep'), may hold values from -4 to 4
Outputs:
- new_master: float32 [2, 32, 8192], P('grp', 'rep')
- new_momentum: float32 [2, 32, 8192], P('grp', 'rep')
- new_params: bfloat16 [2, 32, 8192], P('grp')
The draws below stay inside these ranges and needn't reach their ends.
All inputs are finite; a program needn't handle non-finite values.
Results may differ from the reference program's by a relative error of at most 0.001.
Values may be sent and summed in bfloat16 or wider, within the bound.
A program may use at most 128 MiB of HBM per device.

```python
import jax
import jax.numpy as jnp
from jax import lax

D = 8192
ROWS = 32
REPLICAS = 16
GROUPS = 2


def rough_noise(key, shape):
    return jnp.clip(jax.random.normal(key, shape, jnp.float32), -3.0, 3.0)


def snapshot_base(key):
    key_base = jax.random.fold_in(key, 11)
    base = jnp.clip(jax.random.normal(key_base, (GROUPS, ROWS, D), jnp.float32), -4.0, 4.0)
    return base.astype(jnp.bfloat16)


def drift_scales(key):
    key_rows = jax.random.fold_in(key, 12)
    key_cols = jax.random.fold_in(key, 13)
    row_log = jax.random.uniform(key_rows, (GROUPS, ROWS, 1), jnp.float32, 0.0, 1.0) * jnp.log(10.0)
    col_span = jnp.log(10.0)
    ramp_span = jnp.log(3.0)
    col_log = jax.random.uniform(key_cols, (GROUPS, 1, D), jnp.float32, 0.0, 1.0) * col_span
    position = jnp.arange(ROWS, dtype=jnp.float32).reshape(1, ROWS, 1) / max(ROWS - 1, 1)
    group_pos = jnp.arange(GROUPS, dtype=jnp.float32).reshape(GROUPS, 1, 1) / max(GROUPS - 1, 1)
    row_factor = jnp.exp(row_log + ramp_span * position + jnp.log(3.0) * group_pos)
    return row_factor * jnp.exp(col_log)


def draw_snapshot(key, part):
    return snapshot_base(key)


def draw_local_params(key, part):
    start = snapshot_base(key).astype(jnp.float32)
    scale = drift_scales(key)
    common = 0.005 * rough_noise(jax.random.fold_in(key, 21), (GROUPS, ROWS, D)) * scale
    owners = jax.random.permutation(jax.random.fold_in(key, 23), REPLICAS).astype(jnp.int32)
    row_owner = (jnp.arange(ROWS, dtype=jnp.int32) // (ROWS // REPLICAS)).reshape(1, ROWS, 1)
    own_rate = 0.005
    key_own = jax.random.fold_in(key, 22)

    def one_replica(replica):
        noise = rough_noise(jax.random.fold_in(key_own, replica), (GROUPS, ROWS, D))
        spike = jnp.where(row_owner == owners[replica], 8.0, 1.0)
        return (start + common + own_rate * noise * scale * spike).astype(jnp.bfloat16)
    return lax.map(one_replica, jnp.arange(REPLICAS, dtype=jnp.int32))


def block_levels(key, extent, shards, low, largest):
    def one(dim, parts):
        steps = jax.random.uniform(jax.random.fold_in(jax.random.fold_in(key, 6), dim), (parts,), jnp.float32, low / len(shards), largest / len(shards))
        return jnp.repeat(jnp.exp(steps), extent[dim] // parts).reshape((-1,) + (1,) * (len(extent) - dim - 1))

    factor_of = one(*shards[0])
    for cut in shards[1:]:
        factor_of = factor_of * one(*cut)
    return factor_of


def scatter_about(stream_key, dims, deviation, most, cuts=(), kind=jnp.bfloat16):
    result = jax.random.normal(stream_key, dims, jnp.float32) * deviation
    if len(cuts) > 0:
        result = block_levels(stream_key, dims, cuts, -0.22, 0.18) * result
    return jnp.clip(result, min=-most, max=most).astype(kind)


def setup_inputs(seed: int = 0) -> dict:
    key_list = jax.random.split(jax.random.key(seed), 5)
    local_params = draw_local_params(jax.random.fold_in(key_list[4], 71), 0)
    snapshot = draw_snapshot(jax.random.fold_in(key_list[4], 71), 0)
    master = scatter_about(key_list[2], (GROUPS, ROWS, D), 1.0, 6.0, ((0, 2), (1, 16)), jnp.float32)
    momentum = scatter_about(key_list[3], (GROUPS, ROWS, D), 0.5, 4.0, ((0, 2), (1, 16)), jnp.float32)
    return dict(local_params=local_params, snapshot=snapshot, master=master, momentum=momentum)


nesterov_mu = 0.9
outer_rate = 0.7
clip_limit = 0.15
epsilon = 1e-06

def reference(local_params, snapshot, master, momentum):

    def add_replica(carry, replica):
        return (carry + replica.astype(jnp.float32), None)
    replica_sum, unused = lax.scan(add_replica, jnp.zeros(snapshot.shape, jnp.float32), local_params)
    outer_grad = snapshot.astype(jnp.float32) - replica_sum / REPLICAS
    grad_rms = jnp.sqrt(jnp.sum(outer_grad * outer_grad) / (GROUPS * ROWS * D) + epsilon)
    clipped = jnp.minimum(1.0, clip_limit / grad_rms) * outer_grad
    new_momentum = nesterov_mu * momentum + clipped
    new_master = master - outer_rate * (clipped + nesterov_mu * new_momentum)
    return (new_master, new_momentum, new_master.astype(jnp.bfloat16))
```

```python
import functools

import jax
import jax.numpy as jnp
from jax import lax
from jax.experimental import pallas as pl
from jax.experimental.pallas import tpu as pltpu
from jax.sharding import PartitionSpec as P

nesterov_mu = 0.9
outer_rate = 0.7
clip_limit = 0.15
epsilon = 1e-06

f32 = jnp.float32
bf16 = jnp.bfloat16


def kernel(
    n, groups, own, width, elements,
    local_hbm, snap_hbm, master_hbm, mom_hbm,
    master_out, mom_out, params_out,
    local_v, snap_v, send_v, snap_own, recv_v, acc, grad, master_v, mom_v, gather_v, sq,
    in_sem, rs_send, rs_recv, sq_send, sq_recv, ag_send, ag_recv,
):
    me = lax.axis_index("rep")
    grp = lax.axis_index("grp")
    planes = n // 4
    plane = me // 4
    lane = me % 4
    total = n * groups
    my_id = grp * n + me

    loads = [pltpu.make_async_copy(local_hbm.at[p], local_v.at[p], in_sem.at[p]) for p in range(planes)]
    for c in loads:
        c.start()
    snap_load = pltpu.make_async_copy(snap_hbm.at[plane], snap_v, in_sem.at[planes])
    master_load = pltpu.make_async_copy(master_hbm.at[0], master_v, in_sem.at[planes + 1])
    mom_load = pltpu.make_async_copy(mom_hbm.at[0], mom_v, in_sem.at[planes + 2])
    snap_load.start()
    master_load.start()
    mom_load.start()

    def device(index):
        other = (my_id + index) % total
        return {"rep": other % n, "grp": other // n}

    barrier = pltpu.get_barrier_semaphore()

    @pl.loop(1, total)
    def _(i):
        pl.semaphore_signal(barrier, inc=1, device_id=device(i), device_id_type=pl.DeviceIdType.MESH)

    for p in range(planes):
        loads[p].wait()
        for j in range(4):
            send_v[p * 4 + j] = local_v[p, j * own:(j + 1) * own, :]

    pl.semaphore_wait(barrier, total - 1)

    def scatter(target, source):
        return pltpu.make_async_remote_copy(
            src_ref=send_v.at[target], dst_ref=recv_v.at[source],
            send_sem=rs_send.at[target], recv_sem=rs_recv.at[source],
            device_id={"rep": target, "grp": grp}, device_id_type=pl.DeviceIdType.MESH,
        )

    def offset(k):
        return n // 2 + (1 - 2 * (k % 2)) * ((k + 1) // 2)

    @pl.loop(0, n - 1)
    def _(k):
        scatter((me + offset(k)) % n, me).start()

    snap_load.wait()
    for j in range(4):
        snap_own[j] = snap_v[j * own:(j + 1) * own, :]
    acc[...] = send_v[me].astype(f32)
    master_load.wait()
    mom_load.wait()

    @pl.loop(0, n - 1)
    def _(k):
        source = (me + 2 * n - 1 - k) % n
        pltpu.make_async_remote_copy(
            src_ref=send_v.at[source], dst_ref=recv_v.at[source],
            send_sem=rs_send.at[source], recv_sem=rs_recv.at[source],
            device_id={"rep": source, "grp": grp}, device_id_type=pl.DeviceIdType.MESH,
        ).wait_recv()
        acc[...] += recv_v[source].astype(f32)

    grad[...] = snap_own[lane].astype(f32) - acc[...] * (1.0 / n)
    g2 = grad[...] * grad[...]
    part = g2[:, 0:128]
    for k in range(1, width // 128):
        part = part + g2[:, k * 128:(k + 1) * 128]
    sq[my_id] = jnp.sum(part, axis=0, keepdims=True)

    def share(index):
        slot = (my_id + index) % total
        return pltpu.make_async_remote_copy(
            src_ref=sq.at[my_id], dst_ref=sq.at[my_id],
            send_sem=sq_send.at[slot], recv_sem=sq_recv.at[my_id],
            device_id=device(index), device_id_type=pl.DeviceIdType.MESH,
        )

    @pl.loop(1, total)
    def _(i):
        share(i).start()

    @pl.loop(0, n - 1)
    def _(k):
        scatter((me + 1 + k) % n, me).wait_send()

    @pl.loop(1, total)
    def _(i):
        slot = (my_id + i) % total
        pltpu.make_async_remote_copy(
            src_ref=sq.at[my_id], dst_ref=sq.at[slot],
            send_sem=sq_send.at[slot], recv_sem=sq_recv.at[slot],
            device_id=device(i), device_id_type=pl.DeviceIdType.MESH,
        ).wait_recv()

    squares = jnp.sum(jnp.sum(sq[...], axis=0), axis=1, keepdims=True)
    grad_rms = jnp.sqrt(squares / elements + epsilon)
    scale = jnp.minimum(1.0, clip_limit / grad_rms)
    clipped = scale * grad[...]
    new_momentum = nesterov_mu * mom_v[...] + clipped
    new_master = master_v[...] - outer_rate * (clipped + nesterov_mu * new_momentum)
    gather_v[me] = new_master.astype(bf16)
    master_out[0] = new_master
    mom_out[0] = new_momentum

    row = lane // 2
    core = lane % 2
    twin_row = plane * 4 + (1 - row) * 2 + core
    twin_core = plane * 4 + row * 2 + 1 - core

    def move(block, target, slot):
        return pltpu.make_async_remote_copy(
            src_ref=gather_v.at[block], dst_ref=gather_v.at[block],
            send_sem=ag_send.at[slot], recv_sem=ag_recv.at[block],
            device_id={"rep": target, "grp": grp}, device_id_type=pl.DeviceIdType.MESH,
        )

    def block_of(i, r, c):
        return ((plane + i) % planes) * 4 + r * 2 + c

    for i in range(1, planes):
        move(me, block_of(i, row, core), i).start()
    move(me, twin_row, planes).start()
    move(me, twin_core, 2 * planes).start()
    for i in range(1, planes):
        block = block_of(i, row, core)
        move(block, block, 0).wait_recv()
        move(block, twin_row, planes + i).start()
        move(block, twin_core, 2 * planes + i).start()
    for i in range(planes):
        block = block_of(i, 1 - row, core)
        move(block, block, 0).wait_recv()
        move(block, twin_core, 3 * planes + i).start()
    for i in range(planes):
        for r in (row, 1 - row):
            block = block_of(i, r, 1 - core)
            move(block, block, 0).wait_recv()
        where = (plane + i) % planes
        for j in range(4):
            params_out[where, j * own:(j + 1) * own, :] = gather_v[where * 4 + j]

    @pl.loop(1, n)
    def _(k):
        move(me, twin_core, k).wait_send()

    @pl.loop(1, total)
    def _(i):
        share(i).wait_send()


def solution(mesh):
    n, groups = mesh.shape["rep"], mesh.shape["grp"]

    def body(local_params, snapshot, master, momentum):
        own, width = master.shape[1], master.shape[2]
        planes = n // 4
        span = 4 * own
        any_spec = pl.BlockSpec(memory_space=pl.ANY)
        vmem_spec = pl.BlockSpec(memory_space=pltpu.VMEM)
        new_master, new_momentum, new_params = pl.pallas_call(
            functools.partial(kernel, n, groups, own, width, snapshot.shape[1] * width * groups),
            out_shape=(
                jax.ShapeDtypeStruct(master.shape, f32),
                jax.ShapeDtypeStruct(master.shape, f32),
                jax.ShapeDtypeStruct((planes, span, width), bf16),
            ),
            in_specs=[any_spec] * 4,
            out_specs=(vmem_spec,) * 3,
            scratch_shapes=[
                pltpu.VMEM((planes, span, width), bf16),
                pltpu.VMEM((span, width), bf16),
                pltpu.VMEM((n, own, width), bf16),
                pltpu.VMEM((4, own, width), bf16),
                pltpu.VMEM((n, own, width), bf16),
                pltpu.VMEM((own, width), f32),
                pltpu.VMEM((own, width), f32),
                pltpu.VMEM((own, width), f32),
                pltpu.VMEM((own, width), f32),
                pltpu.VMEM((n, own, width), bf16),
                pltpu.VMEM((n * groups, 1, 128), f32),
                pltpu.SemaphoreType.DMA((planes + 3,)),
                pltpu.SemaphoreType.DMA((n,)),
                pltpu.SemaphoreType.DMA((n,)),
                pltpu.SemaphoreType.DMA((n * groups,)),
                pltpu.SemaphoreType.DMA((n * groups,)),
                pltpu.SemaphoreType.DMA((n,)),
                pltpu.SemaphoreType.DMA((n,)),
            ],
            compiler_params=pltpu.CompilerParams(collective_id=0, has_side_effects=True),
        )(
            local_params.reshape(planes, span, width),
            snapshot.reshape(planes, span, width),
            master,
            momentum,
        )
        return new_master, new_momentum, new_params.reshape(snapshot.shape)

    return jax.shard_map(
        body,
        mesh=mesh,
        in_specs=(
            P("rep", "grp", None, None),
            P("grp", None, None),
            P("grp", "rep", None),
            P("grp", "rep", None),
        ),
        out_specs=(P("grp", "rep", None), P("grp", "rep", None), P("grp", None, None)),
        check_vma=False,
    )
```

```python
import functools

import jax
import jax.numpy as jnp
from jax import lax
from jax.experimental import pallas as pl
from jax.experimental.pallas import tpu as pltpu
from jax.sharding import PartitionSpec as P

nesterov_mu = 0.9
outer_rate = 0.7
clip_limit = 0.15
epsilon = 1e-06

f32 = jnp.float32
bf16 = jnp.bfloat16


MESH = pl.DeviceIdType.MESH


def remote(src, dst, send, recv, rep, grp):
    return pltpu.make_async_remote_copy(
        src_ref=src, dst_ref=dst, send_sem=send, recv_sem=recv,
        device_id={"rep": rep, "grp": grp}, device_id_type=MESH,
    )


def each(count, body):
    if count <= 64:
        for i in range(count):
            body(i)
    else:
        pl.loop(0, count)(body)


def kernel(
    n, groups, own, fold, elements,
    local_hbm, snap_hbm, master_hbm, mom_hbm,
    master_out, mom_out, params_out,
    local_v, snap_v, master_v, mom_v, send_v, snap_own, master_d, mom_d, recv_v, gather_v, sq,
    in_sem, rs_send, rs_recv, sq_send, sq_recv, ag_send, ag_recv,
):
    me = lax.axis_index("rep")
    grp = lax.axis_index("grp")
    planes = n // 4
    plane = lax.div(me, 4)
    lane = lax.rem(me, 4)
    row = lax.div(lane, 2)
    core = lax.rem(lane, 2)
    total = n * groups
    part = send_v.shape[2]

    loads = [pltpu.make_async_copy(local_hbm.at[p], local_v.at[p], in_sem.at[p]) for p in range(planes)]
    for c in loads:
        c.start()
    snap_load = pltpu.make_async_copy(snap_hbm.at[plane], snap_v, in_sem.at[planes])
    master_load = pltpu.make_async_copy(master_hbm.at[0], master_v, in_sem.at[planes + 1])
    mom_load = pltpu.make_async_copy(mom_hbm.at[0], mom_v, in_sem.at[planes + 2])
    snap_load.start()
    master_load.start()
    mom_load.start()

    def rep_at(i):
        return lax.rem(me + i, n)

    def grp_at(i):
        return lax.rem(grp + i, groups)

    def peers(body):
        for g in range(groups):
            if g:
                body(me, grp_at(g))
            each(n - 1, lambda i, g=g: body(rep_at(n - 1 - i), grp_at(g)))

    barrier = pltpu.get_barrier_semaphore()
    peers(lambda r, g: pl.semaphore_signal(barrier, inc=1, device_id={"rep": r, "grp": g}, device_id_type=MESH))

    def rows(q):
        return slice(q * own, (q + 1) * own)

    def cols(q):
        return slice(q * part, (q + 1) * part)

    for p in range(planes):
        loads[p].wait()
        for j in range(4):
            for q in range(fold):
                send_v[p * 4 + j, rows(q), :] = local_v[p, rows(j), cols(q)]

    pl.semaphore_wait(barrier, total - 1)

    def offset(k):
        return n // 2 + (1 - 2 * (k % 2)) * ((k + 1) // 2)

    def scatter(k):
        target = rep_at(offset(k))
        remote(send_v.at[target], recv_v.at[me], rs_send.at[target], rs_recv.at[me], target, grp).start()

    each(n - 1, scatter)

    snap_load.wait()
    master_load.wait()
    mom_load.wait()
    for q in range(fold):
        for j in range(4):
            snap_own[j, rows(q), :] = snap_v[rows(j), cols(q)]
        master_d[rows(q), :] = master_v[:, cols(q)]
        mom_d[rows(q), :] = mom_v[:, cols(q)]

    def add(k, acc):
        source = rep_at(n - offset(k))
        remote(send_v.at[source], recv_v.at[source], rs_send.at[source], rs_recv.at[source], source, grp).wait_recv()
        return acc + recv_v[source].astype(f32)

    acc = send_v[me].astype(f32)
    if n <= 64:
        for k in range(n - 1):
            acc = add(k, acc)
    else:
        acc = lax.fori_loop(0, n - 1, add, acc)

    grad = snap_own[lane].astype(f32) - acc * (1.0 / n)
    g2 = grad * grad
    lanes = g2[:, 0:128]
    for k in range(1, part // 128):
        lanes = lanes + g2[:, k * 128:(k + 1) * 128]
    mine = grp * n + me
    sq[mine] = jnp.sum(lanes, axis=0, keepdims=True)

    def share(r, g):
        slot = g * n + r
        return remote(sq.at[mine], sq.at[mine], sq_send.at[slot], sq_recv.at[mine], r, g)

    def shared(r, g):
        slot = g * n + r
        return remote(sq.at[slot], sq.at[slot], sq_send.at[slot], sq_recv.at[slot], r, g)

    peers(lambda r, g: share(r, g).start())

    base = master_d[...]
    velocity = nesterov_mu * mom_d[...]
    peers(lambda r, g: shared(r, g).wait_recv())

    squares = jnp.sum(jnp.sum(sq[...], axis=0), axis=1, keepdims=True)
    grad_rms = jnp.sqrt(squares / elements + epsilon)
    scale = jnp.minimum(1.0, clip_limit / grad_rms)
    clipped = scale * grad
    new_momentum = velocity + clipped
    new_master = base - outer_rate * (clipped + nesterov_mu * new_momentum)
    gather_v[me] = new_master.astype(bf16)

    twin_row = plane * 4 + (1 - row) * 2 + core
    twin_core = plane * 4 + row * 2 + 1 - core

    def move(block, target, slot):
        return remote(gather_v.at[block], gather_v.at[block], ag_send.at[slot], ag_recv.at[block], target, grp)

    def place(i):
        return lax.rem(plane + i, planes)

    def block_of(i, r, c):
        return place(i) * 4 + r * 2 + c

    def unfold(i, r, c):
        where = place(i)
        for j in range(4):
            @pl.when(r * 2 + c == j)
            def _():
                for q in range(fold):
                    params_out[where, rows(j), cols(q)] = gather_v[where * 4 + j, rows(q), :]

    for i in range(1, planes):
        move(me, block_of(i, row, core), i).start()
    move(me, twin_row, planes).start()
    move(me, twin_core, 2 * planes).start()
    for q in range(fold):
        master_out[0, :, cols(q)] = new_master[rows(q), :]
        mom_out[0, :, cols(q)] = new_momentum[rows(q), :]
    unfold(0, row, core)
    for i in range(1, planes):
        block = block_of(i, row, core)
        move(block, block, 0).wait_recv()
        move(block, twin_row, planes + i).start()
        move(block, twin_core, 2 * planes + i).start()
        unfold(i, row, core)
    for i in range(planes):
        block = block_of(i, 1 - row, core)
        move(block, block, 0).wait_recv()
        move(block, twin_core, 3 * planes + i).start()
        unfold(i, 1 - row, core)
    for i in range(planes):
        for r in (row, 1 - row):
            block = block_of(i, r, 1 - core)
            move(block, block, 0).wait_recv()
            unfold(i, r, 1 - core)

    def drained(k):
        target = rep_at(1 + k)
        remote(send_v.at[target], recv_v.at[me], rs_send.at[target], rs_recv.at[me], target, grp).wait_send()
        move(me, twin_core, 1 + k).wait_send()

    each(n - 1, drained)
    peers(lambda r, g: share(r, g).wait_send())


def store(master_in, mom_in, params_in, master_out, mom_out, params_out, sem):
    copies = [
        pltpu.make_async_copy(params_in, params_out, sem.at[0]),
        pltpu.make_async_copy(master_in, master_out, sem.at[1]),
        pltpu.make_async_copy(mom_in, mom_out, sem.at[2]),
    ]
    for c in copies:
        c.start()
    for c in copies:
        c.wait()


def solution(mesh):
    n, groups = mesh.shape["rep"], mesh.shape["grp"]

    def body(local_params, snapshot, master, momentum):
        own, width = master.shape[1], master.shape[2]
        planes = n // 4
        span = 4 * own
        fold = max(1, 16 // own)
        deep, part = own * fold, width // fold
        hbm_spec = pl.BlockSpec(memory_space=pltpu.HBM)
        vmem_spec = pl.BlockSpec(memory_space=pltpu.VMEM)
        results = pl.pallas_call(
            functools.partial(kernel, n, groups, own, fold, snapshot.shape[1] * width * groups),
            out_shape=(
                pltpu.VMEM(master.shape, f32),
                pltpu.VMEM(master.shape, f32),
                pltpu.VMEM((planes, span, width), bf16),
            ),
            in_specs=[hbm_spec] * 4,
            out_specs=(vmem_spec,) * 3,
            scratch_shapes=[
                pltpu.VMEM((planes, span, width), bf16),
                pltpu.VMEM((span, width), bf16),
                pltpu.VMEM((own, width), f32),
                pltpu.VMEM((own, width), f32),
                pltpu.VMEM((n, deep, part), bf16),
                pltpu.VMEM((4, deep, part), bf16),
                pltpu.VMEM((deep, part), f32),
                pltpu.VMEM((deep, part), f32),
                pltpu.VMEM((n, deep, part), bf16),
                pltpu.VMEM((n, deep, part), bf16),
                pltpu.VMEM((n * groups, 1, 128), f32),
                pltpu.SemaphoreType.DMA((planes + 3,)),
                pltpu.SemaphoreType.DMA((n,)),
                pltpu.SemaphoreType.DMA((n,)),
                pltpu.SemaphoreType.DMA((n * groups,)),
                pltpu.SemaphoreType.DMA((n * groups,)),
                pltpu.SemaphoreType.DMA((n,)),
                pltpu.SemaphoreType.DMA((n,)),
            ],
            compiler_params=pltpu.CompilerParams(
                collective_id=0, has_side_effects=True, vmem_limit_bytes=32 * 2**20
            ),
        )(
            local_params.reshape(planes, span, width),
            snapshot.reshape(planes, span, width),
            master,
            momentum,
        )
        new_master, new_momentum, new_params = pl.pallas_call(
            store,
            out_shape=(
                jax.ShapeDtypeStruct(master.shape, f32),
                jax.ShapeDtypeStruct(master.shape, f32),
                jax.ShapeDtypeStruct((planes, span, width), bf16),
            ),
            in_specs=[vmem_spec] * 3,
            out_specs=(hbm_spec,) * 3,
            scratch_shapes=[pltpu.SemaphoreType.DMA((3,))],
            compiler_params=pltpu.CompilerParams(vmem_limit_bytes=16 * 2**20),
        )(*results)
        return new_master, new_momentum, new_params.reshape(snapshot.shape)

    return jax.shard_map(
        body,
        mesh=mesh,
        in_specs=(
            P("rep", "grp", None, None),
            P("grp", None, None),
            P("grp", "rep", None),
            P("grp", "rep", None),
        ),
        out_specs=(P("grp", "rep", None), P("grp", "rep", None), P("grp", None, None)),
        check_vma=False,
    )
```

```python
import functools

import jax
import jax.numpy as jnp
from jax import lax
from jax.experimental import pallas as pl
from jax.experimental.pallas import tpu as pltpu
from jax.sharding import PartitionSpec as P

nesterov_mu = 0.9
outer_rate = 0.7
clip_limit = 0.15
epsilon = 1e-06

f32 = jnp.float32
bf16 = jnp.bfloat16


MESH = pl.DeviceIdType.MESH


def remote(src, dst, send, recv, rep, grp):
    return pltpu.make_async_remote_copy(
        src_ref=src, dst_ref=dst, send_sem=send, recv_sem=recv,
        device_id={"rep": rep, "grp": grp}, device_id_type=MESH,
    )


def each(count, body):
    if count <= 64:
        for i in range(count):
            body(i)
    else:
        pl.loop(0, count)(body)


def kernel(
    n, groups, own, fold, elements,
    local_hbm, snap_hbm, master_hbm, mom_hbm,
    master_out, mom_out, params_out,
    local_v, snap_v, master_v, mom_v, send_v, snap_own, master_d, mom_d, recv_v, gather_v, sq,
    in_sem, rs_send, rs_recv, sq_send, sq_recv, ag_send, ag_recv,
):
    me = lax.axis_index("rep")
    grp = lax.axis_index("grp")
    planes = n // 4
    plane = lax.div(me, 4)
    lane = lax.rem(me, 4)
    row = lax.div(lane, 2)
    core = lax.rem(lane, 2)
    total = n * groups
    part = send_v.shape[2]

    loads = [pltpu.make_async_copy(local_hbm.at[p], local_v.at[p], in_sem.at[p]) for p in range(planes)]
    for c in loads:
        c.start()
    snap_load = pltpu.make_async_copy(snap_hbm.at[plane], snap_v, in_sem.at[planes])
    master_load = pltpu.make_async_copy(master_hbm.at[0], master_v, in_sem.at[planes + 1])
    mom_load = pltpu.make_async_copy(mom_hbm.at[0], mom_v, in_sem.at[planes + 2])
    snap_load.start()
    master_load.start()
    mom_load.start()

    def rep_at(i):
        return lax.rem(me + i, n)

    def grp_at(i):
        return lax.rem(grp + i, groups)

    def peers(body):
        for g in range(groups):
            if g:
                body(me, grp_at(g))
            each(n - 1, lambda i, g=g: body(rep_at(n - 1 - i), grp_at(g)))

    barrier = pltpu.get_barrier_semaphore()
    peers(lambda r, g: pl.semaphore_signal(barrier, inc=1, device_id={"rep": r, "grp": g}, device_id_type=MESH))

    def rows(q):
        return slice(q * own, (q + 1) * own)

    def cols(q):
        return slice(q * part, (q + 1) * part)

    for p in range(planes):
        loads[p].wait()
        for j in range(4):
            for q in range(fold):
                send_v[p * 4 + j, rows(q), :] = local_v[p, rows(j), cols(q)]

    pl.semaphore_wait(barrier, total - 1)

    def offset(k):
        return n // 2 + (1 - 2 * (k % 2)) * ((k + 1) // 2)

    def scatter(k):
        target = rep_at(offset(k))
        remote(send_v.at[target], recv_v.at[me], rs_send.at[target], rs_recv.at[me], target, grp).start()

    each(n - 1, scatter)

    snap_load.wait()
    master_load.wait()
    mom_load.wait()
    for q in range(fold):
        for j in range(4):
            snap_own[j, rows(q), :] = snap_v[rows(j), cols(q)]
        master_d[rows(q), :] = master_v[:, cols(q)]
        mom_d[rows(q), :] = mom_v[:, cols(q)]

    def add(k, acc):
        source = rep_at(n - offset(k))
        remote(send_v.at[source], recv_v.at[source], rs_send.at[source], rs_recv.at[source], source, grp).wait_recv()
        return acc + recv_v[source].astype(f32)

    acc = send_v[me].astype(f32)
    if n <= 64:
        for k in range(n - 1):
            acc = add(k, acc)
    else:
        acc = lax.fori_loop(0, n - 1, add, acc)

    grad = snap_own[lane].astype(f32) - acc * (1.0 / n)
    g2 = grad * grad
    lanes = g2[:, 0:128]
    for k in range(1, part // 128):
        lanes = lanes + g2[:, k * 128:(k + 1) * 128]
    mine = grp * n + me
    sq[mine] = jnp.sum(lanes, axis=0, keepdims=True)

    def share(r, g):
        slot = g * n + r
        return remote(sq.at[mine], sq.at[mine], sq_send.at[slot], sq_recv.at[mine], r, g)

    def shared(r, g):
        slot = g * n + r
        return remote(sq.at[slot], sq.at[slot], sq_send.at[slot], sq_recv.at[slot], r, g)

    peers(lambda r, g: share(r, g).start())

    base = master_d[...]
    velocity = nesterov_mu * mom_d[...]
    peers(lambda r, g: shared(r, g).wait_recv())

    squares = jnp.sum(jnp.sum(sq[...], axis=0), axis=1, keepdims=True)
    grad_rms = jnp.sqrt(squares / elements + epsilon)
    scale = jnp.minimum(1.0, clip_limit / grad_rms)
    clipped = scale * grad
    new_momentum = velocity + clipped
    new_master = base - outer_rate * (clipped + nesterov_mu * new_momentum)
    gather_v[me] = new_master.astype(bf16)

    twin_row = plane * 4 + (1 - row) * 2 + core
    twin_core = plane * 4 + row * 2 + 1 - core

    def move(block, target, slot):
        return remote(gather_v.at[block], gather_v.at[block], ag_send.at[slot], ag_recv.at[block], target, grp)

    def place(i):
        return lax.rem(plane + i, planes)

    def block_of(i, r, c):
        return place(i) * 4 + r * 2 + c

    def unfold(i, r, c):
        where = place(i)
        for j in range(4):
            @pl.when(r * 2 + c == j)
            def _():
                for q in range(fold):
                    params_out[where, rows(j), cols(q)] = gather_v[where * 4 + j, rows(q), :]

    for i in range(1, planes):
        move(me, block_of(i, row, core), i).start()
    move(me, twin_row, planes).start()
    move(me, twin_core, 2 * planes).start()
    for q in range(fold):
        master_out[0, :, cols(q)] = new_master[rows(q), :]
        mom_out[0, :, cols(q)] = new_momentum[rows(q), :]
    unfold(0, row, core)
    for i in range(1, planes):
        block = block_of(i, row, core)
        move(block, block, 0).wait_recv()
        move(block, twin_row, planes + i).start()
        move(block, twin_core, 2 * planes + i).start()
        unfold(i, row, core)
    for i in range(planes):
        block = block_of(i, 1 - row, core)
        move(block, block, 0).wait_recv()
        move(block, twin_core, 3 * planes + i).start()
        unfold(i, 1 - row, core)
    for i in range(planes):
        for r in (row, 1 - row):
            block = block_of(i, r, 1 - core)
            move(block, block, 0).wait_recv()
            unfold(i, r, 1 - core)

    def drained(k):
        target = rep_at(1 + k)
        remote(send_v.at[target], recv_v.at[me], rs_send.at[target], rs_recv.at[me], target, grp).wait_send()
        move(me, twin_core, 1 + k).wait_send()

    each(n - 1, drained)
    peers(lambda r, g: share(r, g).wait_send())


def store(master_in, mom_in, params_in, master_out, mom_out, params_out, sem):
    copies = [
        pltpu.make_async_copy(params_in, params_out, sem.at[0]),
        pltpu.make_async_copy(master_in, master_out, sem.at[1]),
        pltpu.make_async_copy(mom_in, mom_out, sem.at[2]),
    ]
    for c in copies:
        c.start()
    for c in copies:
        c.wait()


def solution(mesh):
    n, groups = mesh.shape["rep"], mesh.shape["grp"]

    def body(local_params, snapshot, master, momentum):
        own, width = master.shape[1], master.shape[2]
        planes = n // 4
        span = 4 * own
        fold = max(1, 16 // own)
        deep, part = own * fold, width // fold
        results_size = (2 * snapshot.shape[1] + 8 * own) * width
        grant = min(60 * 1024 * 2**10, 63 * 2**20 - results_size)
        hbm_spec = pl.BlockSpec(memory_space=pltpu.HBM)
        vmem_spec = pl.BlockSpec(memory_space=pltpu.VMEM)
        results = pl.pallas_call(
            functools.partial(kernel, n, groups, own, fold, snapshot.shape[1] * width * groups),
            out_shape=(
                pltpu.VMEM(master.shape, f32),
                pltpu.VMEM(master.shape, f32),
                pltpu.VMEM((planes, span, width), bf16),
            ),
            in_specs=[hbm_spec] * 4,
            out_specs=(vmem_spec,) * 3,
            scratch_shapes=[
                pltpu.VMEM((planes, span, width), bf16),
                pltpu.VMEM((span, width), bf16),
                pltpu.VMEM((own, width), f32),
                pltpu.VMEM((own, width), f32),
                pltpu.VMEM((n, deep, part), bf16),
                pltpu.VMEM((4, deep, part), bf16),
                pltpu.VMEM((deep, part), f32),
                pltpu.VMEM((deep, part), f32),
                pltpu.VMEM((n, deep, part), bf16),
                pltpu.VMEM((n, deep, part), bf16),
                pltpu.VMEM((n * groups, 1, 128), f32),
                pltpu.SemaphoreType.DMA((planes + 3,)),
                pltpu.SemaphoreType.DMA((n,)),
                pltpu.SemaphoreType.DMA((n,)),
                pltpu.SemaphoreType.DMA((n * groups,)),
                pltpu.SemaphoreType.DMA((n * groups,)),
                pltpu.SemaphoreType.DMA((n,)),
                pltpu.SemaphoreType.DMA((n,)),
            ],
            compiler_params=pltpu.CompilerParams(
                collective_id=0, has_side_effects=True, vmem_limit_bytes=grant
            ),
        )(
            local_params.reshape(planes, span, width),
            snapshot.reshape(planes, span, width),
            master,
            momentum,
        )
        new_master, new_momentum, new_params = pl.pallas_call(
            store,
            out_shape=(
                jax.ShapeDtypeStruct(master.shape, f32),
                jax.ShapeDtypeStruct(master.shape, f32),
                jax.ShapeDtypeStruct((planes, span, width), bf16),
            ),
            in_specs=[vmem_spec] * 3,
            out_specs=(hbm_spec,) * 3,
            scratch_shapes=[pltpu.SemaphoreType.DMA((3,))],
            compiler_params=pltpu.CompilerParams(vmem_limit_bytes=16 * 2**20),
        )(*results)
        return new_master, new_momentum, new_params.reshape(snapshot.shape)

    return jax.shard_map(
        body,
        mesh=mesh,
        in_specs=(
            P("rep", "grp", None, None),
            P("grp", None, None),
            P("grp", "rep", None),
            P("grp", "rep", None),
        ),
        out_specs=(P("grp", "rep", None), P("grp", "rep", None), P("grp", None, None)),
        check_vma=False,
    )
```

```python
import functools

import jax
import jax.numpy as jnp
from jax import lax
from jax.experimental import pallas as pl
from jax.experimental.pallas import tpu as pltpu
from jax.sharding import PartitionSpec as P

nesterov_mu = 0.9
outer_rate = 0.7
clip_limit = 0.15
epsilon = 1e-06

f32 = jnp.float32
bf16 = jnp.bfloat16


MESH = pl.DeviceIdType.MESH


def remote(src, dst, send, recv, rep, grp):
    return pltpu.make_async_remote_copy(
        src_ref=src, dst_ref=dst, send_sem=send, recv_sem=recv,
        device_id={"rep": rep, "grp": grp}, device_id_type=MESH,
    )


def each(count, body):
    if count <= 64:
        for i in range(count):
            body(i)
    else:
        pl.loop(0, count)(body)


def kernel(
    n, groups, own, fold, elements,
    local_hbm, snap_hbm, master_hbm, mom_hbm,
    master_out, mom_out, params_out,
    local_v, snap_v, master_v, mom_v, send_v, snap_own, master_d, mom_d, recv_v, part_v, sum_v, far_v, gather_v, sq,
    in_sem, ready, part_send, part_recv, far_send, far_recv, rs_send, rs_recv, sq_send, sq_recv, ag_send, ag_recv,
):
    me = lax.axis_index("rep")
    grp = lax.axis_index("grp")
    planes = n // 4
    plane = lax.div(me, 4)
    lane = lax.rem(me, 4)
    row = lax.div(lane, 2)
    core = lax.rem(lane, 2)
    total = n * groups
    part = send_v.shape[2]

    loads = [pltpu.make_async_copy(local_hbm.at[p], local_v.at[p], in_sem.at[p]) for p in range(planes)]
    for c in loads:
        c.start()
    snap_load = pltpu.make_async_copy(snap_hbm.at[plane], snap_v, in_sem.at[planes])
    master_load = pltpu.make_async_copy(master_hbm.at[0], master_v, in_sem.at[planes + 1])
    mom_load = pltpu.make_async_copy(mom_hbm.at[0], mom_v, in_sem.at[planes + 2])
    snap_load.start()
    master_load.start()
    mom_load.start()

    def rep_at(i):
        return lax.rem(me + i, n)

    def grp_at(i):
        return lax.rem(grp + i, groups)

    def peers(body):
        for g in range(groups):
            if g:
                body(me, grp_at(g))
            each(n - 1, lambda i, g=g: body(rep_at(n - 1 - i), grp_at(g)))

    barrier = pltpu.get_barrier_semaphore()

    def greet(semaphore, r, g):
        pl.semaphore_signal(semaphore, inc=1, device_id={"rep": r, "grp": g}, device_id_type=MESH)

    each(n - 1, lambda i: greet(barrier, rep_at(n - 1 - i), grp))
    for g in range(1, groups):
        greet(barrier, me, grp_at(g))

    def rows(q):
        return slice(q * own, (q + 1) * own)

    def cols(q):
        return slice(q * part, (q + 1) * part)

    for p in range(planes):
        loads[p].wait()
        for j in range(4):
            for q in range(fold):
                send_v[p * 4 + j, rows(q), :] = local_v[p, rows(j), cols(q)]

    pl.semaphore_wait(barrier, n - 1 + groups - 1)
    for g in range(1, groups):
        greet(ready, me, grp_at(g))

    def place(i):
        return lax.rem(plane + i, planes)

    def lane_at(d):
        return lax.rem(lane + d, 4)

    def collect(i, d):
        to = lane_at(d)
        return remote(send_v.at[place(i) * 4 + to], part_v.at[i, lane], part_send.at[i, to], part_recv.at[i, lane], plane * 4 + to, grp)

    def collected(i, d):
        source = lane_at(4 - d)
        return remote(send_v.at[0], part_v.at[i, source], part_send.at[i, source], part_recv.at[i, source], plane * 4 + source, grp)

    def forward(i):
        return remote(sum_v.at[i], far_v.at[i], far_send.at[i], far_recv.at[i], place(i) * 4 + lane, grp)

    def scatter(i, d):
        target = place(i) * 4 + lane_at(d)
        return remote(send_v.at[target], recv_v.at[i, lane], rs_send.at[i, lane_at(d)], rs_recv.at[i, lane], target, grp)

    def scattered(i, d):
        source = lane_at(4 - d)
        return remote(send_v.at[0], recv_v.at[i, source], rs_send.at[i, source], rs_recv.at[i, source], place(planes - i) * 4 + source, grp)

    direct = [(i, d) for i in (1, 0) for d in range(4) if i or d]
    for i in range(2, planes):
        for d in (1, 2, 3):
            collect(i, d).start()
    for i, d in direct:
        scatter(i, d).start()
    for i in range(2, planes):
        both = send_v[place(i) * 4 + lane].astype(f32)
        for d in (1, 2, 3):
            collected(i, d).wait_recv()
            both = both + part_v[i, lane_at(4 - d)].astype(f32)
        sum_v[i] = both
        forward(i).start()

    snap_load.wait()
    master_load.wait()
    mom_load.wait()
    for q in range(fold):
        for j in range(4):
            snap_own[j, rows(q), :] = snap_v[rows(j), cols(q)]
        master_d[rows(q), :] = master_v[:, cols(q)]
        mom_d[rows(q), :] = mom_v[:, cols(q)]

    acc = send_v[me].astype(f32)
    for i, d in reversed(direct):
        scattered(i, d).wait_recv()
        acc = acc + recv_v[i, lane_at(4 - d)].astype(f32)
    for i in range(2, planes):
        forward(i).wait_recv()
        acc = acc + far_v[i]

    grad = snap_own[lane].astype(f32) - acc * (1.0 / n)
    g2 = grad * grad
    lanes = g2[:, 0:128]
    for k in range(1, part // 128):
        lanes = lanes + g2[:, k * 128:(k + 1) * 128]
    mine = grp * n + me
    sq[mine] = jnp.sum(lanes, axis=0, keepdims=True)

    def share(r, g):
        slot = g * n + r
        return remote(sq.at[mine], sq.at[mine], sq_send.at[slot], sq_recv.at[mine], r, g)

    def shared(r, g):
        slot = g * n + r
        return remote(sq.at[slot], sq.at[slot], sq_send.at[slot], sq_recv.at[slot], r, g)

    pl.semaphore_wait(ready, groups - 1)
    peers(lambda r, g: share(r, g).start())

    base = master_d[...]
    velocity = nesterov_mu * mom_d[...]
    peers(lambda r, g: shared(r, g).wait_recv())

    squares = jnp.sum(jnp.sum(sq[...], axis=0), axis=1, keepdims=True)
    grad_rms = jnp.sqrt(squares / elements + epsilon)
    scale = jnp.minimum(1.0, clip_limit / grad_rms)
    clipped = scale * grad
    new_momentum = velocity + clipped
    new_master = base - outer_rate * (clipped + nesterov_mu * new_momentum)
    gather_v[me] = new_master.astype(bf16)

    twin_row = plane * 4 + (1 - row) * 2 + core
    twin_core = plane * 4 + row * 2 + 1 - core

    def move(block, target, slot):
        return remote(gather_v.at[block], gather_v.at[block], ag_send.at[slot], ag_recv.at[block], target, grp)

    def block_of(i, r, c):
        return place(i) * 4 + r * 2 + c

    def unfold(i, r, c):
        where = place(i)
        for j in range(4):
            @pl.when(r * 2 + c == j)
            def _():
                for q in range(fold):
                    params_out[where, rows(j), cols(q)] = gather_v[where * 4 + j, rows(q), :]

    for i in range(1, planes):
        move(me, block_of(i, row, core), i).start()
    move(me, twin_row, planes).start()
    move(me, twin_core, 2 * planes).start()
    for q in range(fold):
        master_out[0, :, cols(q)] = new_master[rows(q), :]
        mom_out[0, :, cols(q)] = new_momentum[rows(q), :]
    unfold(0, row, core)
    for i in range(1, planes):
        block = block_of(i, row, core)
        move(block, block, 0).wait_recv()
        move(block, twin_row, planes + i).start()
        move(block, twin_core, 2 * planes + i).start()
        unfold(i, row, core)
    for i in range(planes):
        block = block_of(i, 1 - row, core)
        move(block, block, 0).wait_recv()
        move(block, twin_core, 3 * planes + i).start()
        unfold(i, 1 - row, core)
    for i in range(planes):
        for r in (row, 1 - row):
            block = block_of(i, r, 1 - core)
            move(block, block, 0).wait_recv()
            unfold(i, r, 1 - core)

    for i in range(2, planes):
        for d in (1, 2, 3):
            collect(i, d).wait_send()
        forward(i).wait_send()
    for i, d in direct:
        scatter(i, d).wait_send()

    def drained(k):
        move(me, twin_core, 1 + k).wait_send()

    each(n - 1, drained)
    peers(lambda r, g: share(r, g).wait_send())


def store(master_in, mom_in, params_in, master_out, mom_out, params_out, sem):
    copies = [
        pltpu.make_async_copy(params_in, params_out, sem.at[0]),
        pltpu.make_async_copy(master_in, master_out, sem.at[1]),
        pltpu.make_async_copy(mom_in, mom_out, sem.at[2]),
    ]
    for c in copies:
        c.start()
    for c in copies:
        c.wait()


def solution(mesh):
    n, groups = mesh.shape["rep"], mesh.shape["grp"]

    def body(local_params, snapshot, master, momentum):
        own, width = master.shape[1], master.shape[2]
        planes = n // 4
        span = 4 * own
        fold = max(1, 16 // own)
        deep, part = own * fold, width // fold
        results_size = (2 * snapshot.shape[1] + 8 * own) * width
        grant = min(60 * 1024 * 2**10, 63 * 2**20 - results_size)
        hbm_spec = pl.BlockSpec(memory_space=pltpu.HBM)
        vmem_spec = pl.BlockSpec(memory_space=pltpu.VMEM)
        results = pl.pallas_call(
            functools.partial(kernel, n, groups, own, fold, snapshot.shape[1] * width * groups),
            out_shape=(
                pltpu.VMEM(master.shape, f32),
                pltpu.VMEM(master.shape, f32),
                pltpu.VMEM((planes, span, width), bf16),
            ),
            in_specs=[hbm_spec] * 4,
            out_specs=(vmem_spec,) * 3,
            scratch_shapes=[
                pltpu.VMEM((planes, span, width), bf16),
                pltpu.VMEM((span, width), bf16),
                pltpu.VMEM((own, width), f32),
                pltpu.VMEM((own, width), f32),
                pltpu.VMEM((n, deep, part), bf16),
                pltpu.VMEM((4, deep, part), bf16),
                pltpu.VMEM((deep, part), f32),
                pltpu.VMEM((deep, part), f32),
                pltpu.VMEM((2, 4, deep, part), bf16),
                pltpu.VMEM((planes, 4, deep, part), bf16),
                pltpu.VMEM((planes, deep, part), f32),
                pltpu.VMEM((planes, deep, part), f32),
                pltpu.VMEM((n, deep, part), bf16),
                pltpu.VMEM((n * groups, 1, 128), f32),
                pltpu.SemaphoreType.DMA((planes + 3,)),
                pltpu.SemaphoreType.REGULAR,
                pltpu.SemaphoreType.DMA((planes, 4)),
                pltpu.SemaphoreType.DMA((planes, 4)),
                pltpu.SemaphoreType.DMA((planes,)),
                pltpu.SemaphoreType.DMA((planes,)),
                pltpu.SemaphoreType.DMA((2, 4)),
                pltpu.SemaphoreType.DMA((2, 4)),
                pltpu.SemaphoreType.DMA((n * groups,)),
                pltpu.SemaphoreType.DMA((n * groups,)),
                pltpu.SemaphoreType.DMA((n,)),
                pltpu.SemaphoreType.DMA((n,)),
            ],
            compiler_params=pltpu.CompilerParams(
                collective_id=0, has_side_effects=True, vmem_limit_bytes=grant
            ),
        )(
            local_params.reshape(planes, span, width),
            snapshot.reshape(planes, span, width),
            master,
            momentum,
        )
        new_master, new_momentum, new_params = pl.pallas_call(
            store,
            out_shape=(
                jax.ShapeDtypeStruct(master.shape, f32),
                jax.ShapeDtypeStruct(master.shape, f32),
                jax.ShapeDtypeStruct((planes, span, width), bf16),
            ),
            in_specs=[vmem_spec] * 3,
            out_specs=(hbm_spec,) * 3,
            scratch_shapes=[pltpu.SemaphoreType.DMA((3,))],
            compiler_params=pltpu.CompilerParams(vmem_limit_bytes=16 * 2**20),
        )(*results)
        return new_master, new_momentum, new_params.reshape(snapshot.shape)

    return jax.shard_map(
        body,
        mesh=mesh,
        in_specs=(
            P("rep", "grp", None, None),
            P("grp", None, None),
            P("grp", "rep", None),
            P("grp", "rep", None),
        ),
        out_specs=(P("grp", "rep", None), P("grp", "rep", None), P("grp", None, None)),
        check_vma=False,
    )
```
